32 devices in a mesh: gx: 4 (over x, core), gy: 4 (over z), gz: 2 (over y).
Axes of the slice: x: 2, y: 2, z: 4, core: 2. Of those that a mesh axis runs over, the one named last changes fastest.
Arguments:
- velocity: float32 [3, 64, 128, 256], P(None, 'gx', 'gy', 'gz'), may hold values from -4 to 4
- plane_early: float32 [3, 128, 256], P(None, 'gy', 'gx'), may hold values from -4 to 4
- plane_late: float32 [3, 128, 256], P(None, 'gy', 'gx'), may hold values from -4 to 4
- blend: float32 [1], replicated, may hold values from 0 to 1
Outputs:
- advanced: float32 [3, 64, 128, 256], P(None, 'gx', 'gy', 'gz')
The draws below stay inside these ranges and needn't reach their ends.
All inputs are finite; a program needn't handle non-finite values.
Results may differ from the reference program's by a relative error of at most 0.00002.
Values sent between devices are 32-bit elements; how exact they have to be, the bound alone decides.
A program may use at most 64 MiB of HBM per device.

```python
import jax
import jax.numpy as jnp

STEPS = 4
NX = 64
NY = 128
NZ = 256


def steps_of(stream_key, extent, pieces, smallest, top_value):
    factor_of, own = 1.0, jax.random.fold_in(stream_key, 6)
    for position, shards_of in pieces:
        heights = jnp.exp(jax.random.uniform(jax.random.fold_in(own, position), (shards_of,), jnp.float32, smallest / len(pieces), top_value / len(pieces)))
        factor_of = factor_of * jnp.repeat(heights, extent[position] // shards_of).reshape([-1 if axis == position else 1 for axis in range(len(extent))])
    return factor_of


def normal_values(key, extent, spread, bound, cuts=(), held_as=jnp.bfloat16):
    array = spread * jax.random.normal(key, extent, jnp.float32)
    if cuts:
        array = array * steps_of(key, extent, cuts, -0.22, 0.18)
    return jnp.clip(array, -bound, bound).astype(held_as)


def setup_inputs(seed: int = 0) -> dict:
    arg_keys = jax.random.split(jax.random.key(seed), 5)
    return {
        "velocity": normal_values(arg_keys[0], (3, NX, NY, NZ), 1.0, 4.0, ((1, 4), (2, 4), (3, 2)), jnp.float32),
        "plane_early": normal_values(arg_keys[1], (3, NY, NZ), 1.0, 4.0, ((1, 4), (2, 4)), jnp.float32),
        "plane_late": normal_values(arg_keys[2], (3, NY, NZ), 1.0, 4.0, ((1, 4), (2, 4)), jnp.float32),
        "blend": jnp.clip(jax.random.uniform(arg_keys[3], (1,), jnp.float32, 0.0, 1.0), 0.0, 1.0),
    }


courant = 0.08


def advect(padded):
    center = padded[:, 1:-1, 1:-1, 1:-1]
    stream_u = center[0:1]
    span_v = center[1:2]
    vert_w = center[2:3]
    back_x = center - padded[:, :-2, 1:-1, 1:-1]
    ahead_x = padded[:, 2:, 1:-1, 1:-1] - center
    back_y = center - padded[:, 1:-1, :-2, 1:-1]
    ahead_y = padded[:, 1:-1, 2:, 1:-1] - center
    back_z = center - padded[:, 1:-1, 1:-1, :-2]
    ahead_z = padded[:, 1:-1, 1:-1, 2:] - center
    tendency = (jnp.maximum(stream_u, 0.0) * back_x + jnp.minimum(stream_u, 0.0) * ahead_x) \
        + (jnp.maximum(span_v, 0.0) * back_y + jnp.minimum(span_v, 0.0) * ahead_y) \
        + (jnp.maximum(vert_w, 0.0) * back_z + jnp.minimum(vert_w, 0.0) * ahead_z)
    return center - courant * tendency


def reference(velocity, plane_early, plane_late, blend):
    weight = blend[0]
    inflow = (1.0 - weight) * plane_early + weight * plane_late
    inflow_span = jnp.concatenate([inflow[:, -1:], inflow, inflow[:, :1]], axis=1)
    current = velocity
    for substep in range(STEPS):
        padded = jnp.concatenate([current[:, :, -1:], current, current[:, :, :1]], axis=2)
        empty_slab = jnp.zeros_like(inflow_span)[:, None]
        padded = jnp.concatenate([inflow_span[:, None], padded, empty_slab], axis=1)
        padded = jnp.pad(padded, ((0, 0), (0, 0), (0, 0), (1, 1)))
        current = advect(padded)
    return current
```

```python
import functools

import jax
import jax.numpy as jnp
from jax import lax
from jax.experimental import pallas as pl
from jax.experimental.pallas import tpu as pltpu
from jax.sharding import PartitionSpec as P

STEPS = 4
COURANT = 0.08
TOP = 8

MESH = pl.DeviceIdType.MESH


def kernel(sizes, vel_hbm, early_hbm, late_hbm, blend_ref, out_ref,
           cur, early, late, inflow_send, inflow_recv,
           y_send, y_recv, z_send, z_low, z_high,
           load_sem, xs, xr, ys, yr, zs, zr, fs, fr):
    nx, ny, nz = sizes
    comps, cells_x, cells_y, cells_z = vel_hbm.shape
    share = nx // nz
    piece = early_hbm.shape[2]
    gx, gy, gz = (lax.axis_index(name) for name in ("gx", "gy", "gz"))
    own = pl.ds(TOP, cells_y)

    load_v = pltpu.make_async_copy(
        vel_hbm, cur.at[0, :, pl.ds(1, cells_x), own, :], load_sem.at[0])
    load_e = pltpu.make_async_copy(early_hbm, early, load_sem.at[1])
    load_l = pltpu.make_async_copy(late_hbm, late, load_sem.at[2])
    load_v.start()
    load_e.start()
    load_l.start()

    has_left, has_right = gx > 0, gx < nx - 1
    has_below, has_above = gz > 0, gz < nz - 1
    feeds = (gz == gx // share) & (gx != 0)
    y_up = {"gy": lax.rem(gy + 1, ny)}
    y_down = {"gy": lax.rem(gy + ny - 1, ny)}

    barrier = pltpu.get_barrier_semaphore()
    peers = [
        (has_left, {"gx": gx - 1}),
        (has_right, {"gx": gx + 1}),
        (has_below, {"gz": gz - 1}),
        (has_above, {"gz": gz + 1}),
        (feeds, {"gx": 0}),
    ]
    for k in range(share):
        source = gz * share + k
        peers.append(((gx == 0) & (source != 0), {"gx": source}))
    expected = jnp.int32(2)
    for where in (y_up, y_down):
        pl.semaphore_signal(barrier, 1, device_id=where, device_id_type=MESH)
    for present, where in peers:
        @pl.when(present)
        def _(where=where):
            pl.semaphore_signal(barrier, 1, device_id=where, device_id_type=MESH)
        expected = expected + jnp.where(present, 1, 0)

    def remote(src, dst, send, recv, where):
        return pltpu.make_async_remote_copy(
            src_ref=src, dst_ref=dst, send_sem=send, recv_sem=recv,
            device_id=where, device_id_type=MESH)

    def x_copies(t):
        return [
            (has_right, has_left, remote(
                cur.at[t, :, cells_x, own, :], cur.at[t, :, 0, own, :],
                xs.at[t, 0], xr.at[t, 0], {"gx": gx + 1})),
            (has_left, has_right, remote(
                cur.at[t, :, 1, own, :], cur.at[t, :, cells_x + 1, own, :],
                xs.at[t, 1], xr.at[t, 1], {"gx": gx - 1})),
        ]

    def y_copies(t):
        return [
            remote(y_send.at[t, 1], y_recv.at[t, 0], ys.at[t, 0], yr.at[t, 0], y_up),
            remote(y_send.at[t, 0], y_recv.at[t, 1], ys.at[t, 1], yr.at[t, 1], y_down),
        ]

    def z_copies(t):
        return [
            (has_above, has_below, remote(
                z_send.at[t], z_low.at[t], zs.at[t, 0], zr.at[t, 0], {"gz": gz + 1})),
            (has_below, has_above, remote(
                z_send.at[t], z_high.at[t], zs.at[t, 1], zr.at[t, 1], {"gz": gz - 1})),
        ]

    lane = lax.broadcasted_iota(jnp.int32, (cells_y, cells_z), 1)

    def pack(t, x, planes, acc):
        for c in range(comps):
            j = c * cells_x + x
            y_send[t, 0, j] = planes[c][0:1, :]
            y_send[t, 1, j] = planes[c][cells_y - 1:cells_y, :]
            turned = pltpu.roll(planes[c], (2 * j + 1) % cells_z, 1)
            acc = jnp.where(lane // 2 == j, turned, acc)
        return acc

    def start_x(t):
        for sends, _, copy in x_copies(t):
            pl.when(sends)(copy.start)

    def start_yz(t):
        for copy in y_copies(t):
            copy.start()
        for sends, _, copy in z_copies(t):
            pl.when(sends)(copy.start)

    for t in range(STEPS):
        @pl.when(gx == nx - 1)
        def _(t=t):
            cur[t, :, cells_x + 1, own, :] = jnp.zeros((comps, cells_y, cells_z), jnp.float32)

        @pl.when(gz == 0)
        def _(t=t):
            z_low[t] = jnp.zeros((cells_y, cells_z), jnp.float32)

        @pl.when(gz == nz - 1)
        def _(t=t):
            z_high[t] = jnp.zeros((cells_y, cells_z), jnp.float32)

    load_e.wait()
    load_l.wait()
    weight = blend_ref[0]

    def blended():
        mixed = (1.0 - weight) * early[...] + weight * late[...]
        return jnp.concatenate([mixed] * share, axis=2)

    feed = [remote(inflow_send, inflow_recv.at[k], fs.at[k], fr.at[k], {"gx": 0})
            for k in range(share)]

    @pl.when(feeds)
    def _():
        inflow_send[...] = blended()

    @pl.when((gx == 0) & (gz == 0))
    def _():
        inflow_recv[0] = blended()

    load_v.wait()
    pl.semaphore_wait(barrier, expected)
    start_x(0)

    def first(x, acc):
        return pack(0, x, [cur[0, c, x + 1, own, :] for c in range(comps)], acc)

    zero = jnp.zeros((cells_y, cells_z), jnp.float32)
    z_send[0] = lax.fori_loop(0, cells_x, first, zero)
    start_yz(0)
    for k in range(share):
        @pl.when(feeds & (lax.rem(gx, share) == k))
        def _(k=k):
            feed[k].start()

    def update(t, x, halo):
        q = [cur[t, c, x + 1, own, :] for c in range(comps)]
        ahead, back = [], []
        keep = jnp.float32(1.0)
        for c in range(comps):
            scaled = COURANT * q[c]
            back.append(jnp.maximum(scaled, 0.0))
            ahead.append(back[c] - scaled)
            keep = keep - jnp.abs(scaled)
        result = []
        for c in range(comps):
            j = c * cells_x + x
            edge = pltpu.roll(halo, lax.rem(2 * cells_z - 2 * j, cells_z), 1)
            z_prev = jnp.where(lane == 0, edge, pltpu.roll(q[c], 1, 1))
            z_next = jnp.where(lane == cells_z - 1, edge, pltpu.roll(q[c], cells_z - 1, 1))
            x_part = back[0] * cur[t, c, x, own, :] + ahead[0] * cur[t, c, x + 2, own, :]
            y_part = (back[1] * cur[t, c, x + 1, pl.ds(TOP - 1, cells_y), :]
                      + ahead[1] * cur[t, c, x + 1, pl.ds(TOP + 1, cells_y), :])
            z_part = back[2] * z_prev + ahead[2] * z_next
            result.append(keep * q[c] + (x_part + (y_part + z_part)))
        return result

    for t in range(STEPS):
        for _, recvs, copy in z_copies(t):
            pl.when(recvs)(copy.wait_recv)
        for copy in y_copies(t):
            copy.wait_recv()

        def place(x, carry, t=t):
            for c in range(comps):
                j = c * cells_x + x
                cur[t, c, x + 1, TOP - 1:TOP, :] = y_recv[t, 0, j]
                cur[t, c, x + 1, TOP + cells_y:TOP + cells_y + 1, :] = y_recv[t, 1, j]
            return carry

        lax.fori_loop(0, cells_x, place, 0)
        halo = jnp.where(lane % 2 == 0, z_low[t], pltpu.roll(z_high[t], cells_z - 2, 1))
        for _, recvs, copy in x_copies(t):
            pl.when(recvs)(copy.wait_recv)
        if t == 0:
            @pl.when(gx == 0)
            def _():
                for k in range(share):
                    @pl.when(gz * share + k != 0)
                    def _(k=k):
                        feed[k].wait_recv()
                for c in range(comps):
                    plane = inflow_recv[0, c]
                    for k in range(1, share):
                        plane = jnp.where(lane // piece == k, inflow_recv[k, c], plane)
                    for s in range(STEPS):
                        cur[s, c, 0, own, :] = plane

        if t == STEPS - 1:
            def last(x, carry, t=t, halo=halo):
                fresh = update(t, x, halo)
                for c in range(comps):
                    out_ref[c, x] = fresh[c]
                return carry

            lax.fori_loop(0, cells_x, last, 0)
        else:
            def advance(x, acc, t=t, halo=halo):
                fresh = update(t, x, halo)
                for c in range(comps):
                    cur[t + 1, c, x + 1, own, :] = fresh[c]
                return pack(t + 1, x, fresh, acc)

            acc = advance(cells_x - 1, advance(0, zero))
            start_x(t + 1)
            z_send[t + 1] = lax.fori_loop(1, cells_x - 1, advance, acc)
            start_yz(t + 1)

    for t in range(STEPS):
        for sends, _, copy in x_copies(t):
            pl.when(sends)(copy.wait_send)
        for copy in y_copies(t):
            copy.wait_send()
        for sends, _, copy in z_copies(t):
            pl.when(sends)(copy.wait_send)
    for k in range(share):
        @pl.when(feeds & (lax.rem(gx, share) == k))
        def _(k=k):
            feed[k].wait_send()


def local(sizes, velocity, plane_early, plane_late, blend):
    comps, cells_x, cells_y, cells_z = velocity.shape
    nx, ny, nz = sizes
    assert nx % nz == 0 and cells_z == 128 and 2 * comps * cells_x <= cells_z
    share = nx // nz
    planes = comps * cells_x
    block = (comps, cells_y, cells_z)
    dma = pltpu.SemaphoreType.DMA
    return pl.pallas_call(
        functools.partial(kernel, sizes),
        out_shape=jax.ShapeDtypeStruct(velocity.shape, velocity.dtype),
        in_specs=[pl.BlockSpec(memory_space=pl.ANY)] * 3
        + [pl.BlockSpec(memory_space=pltpu.SMEM)],
        out_specs=pl.BlockSpec(memory_space=pltpu.VMEM),
        scratch_shapes=[
            pltpu.VMEM((STEPS, comps, cells_x + 2, cells_y + 2 * TOP, cells_z), jnp.float32),
            pltpu.VMEM(plane_early.shape, jnp.float32),
            pltpu.VMEM(plane_late.shape, jnp.float32),
            pltpu.VMEM(block, jnp.float32),
            pltpu.VMEM((share,) + block, jnp.float32),
            pltpu.VMEM((STEPS, 2, planes, 1, cells_z), jnp.float32),
            pltpu.VMEM((STEPS, 2, planes, 1, cells_z), jnp.float32),
            pltpu.VMEM((STEPS, cells_y, cells_z), jnp.float32),
            pltpu.VMEM((STEPS, cells_y, cells_z), jnp.float32),
            pltpu.VMEM((STEPS, cells_y, cells_z), jnp.float32),
            dma((3,)),
            dma((STEPS, 2)), dma((STEPS, 2)),
            dma((STEPS, 2)), dma((STEPS, 2)),
            dma((STEPS, 2)), dma((STEPS, 2)),
            dma((share,)), dma((share,)),
        ],
        compiler_params=pltpu.CompilerParams(collective_id=0, has_side_effects=True),
        name="advect_substeps",
    )(velocity, plane_early, plane_late, blend)


def solution(mesh):
    sizes = tuple(mesh.shape[name] for name in ("gx", "gy", "gz"))
    return jax.shard_map(
        functools.partial(local, sizes),
        mesh=mesh,
        in_specs=(P(None, "gx", "gy", "gz"), P(None, "gy", "gx"), P(None, "gy", "gx"), P()),
        out_specs=P(None, "gx", "gy", "gz"),
        check_vma=False,
    )
```

```python
import functools

import jax
import jax.numpy as jnp
from jax import lax
from jax.experimental import pallas as pl
from jax.experimental.pallas import tpu as pltpu
from jax.sharding import PartitionSpec as P

STEPS = 4
COURANT = 0.08
UNROLL = 7
TOP = 8

MESH = pl.DeviceIdType.MESH


def kernel(sizes, vel_hbm, early_hbm, late_hbm, blend_ref, out_ref,
           cur, early, late, inflow_send, inflow_recv,
           y_send, y_recv, z_send, z_low, z_high,
           load_sem, xs, xr, ys, yr, zs, zr, fs, fr):
    nx, ny, nz = sizes
    comps, cells_x, cells_y, cells_z = vel_hbm.shape
    share = nx // nz
    piece = early_hbm.shape[2]
    gx, gy, gz = (lax.axis_index(name) for name in ("gx", "gy", "gz"))
    own = pl.ds(TOP, cells_y)

    load_v = pltpu.make_async_copy(
        vel_hbm, cur.at[0, :, pl.ds(1, cells_x), own, :], load_sem.at[0])
    load_e = pltpu.make_async_copy(early_hbm, early, load_sem.at[1])
    load_l = pltpu.make_async_copy(late_hbm, late, load_sem.at[2])
    load_v.start()
    load_e.start()
    load_l.start()

    has_left, has_right = gx > 0, gx < nx - 1
    has_below, has_above = gz > 0, gz < nz - 1
    feeds = (gz == gx // share) & (gx != 0)
    y_up = {"gy": lax.rem(gy + 1, ny)}
    y_down = {"gy": lax.rem(gy + ny - 1, ny)}

    barrier = pltpu.get_barrier_semaphore()
    peers = [
        (has_left, {"gx": gx - 1}),
        (has_right, {"gx": gx + 1}),
        (has_below, {"gz": gz - 1}),
        (has_above, {"gz": gz + 1}),
        (feeds, {"gx": 0}),
    ]
    for k in range(share):
        source = gz * share + k
        peers.append(((gx == 0) & (source != 0), {"gx": source}))
    expected = jnp.int32(2)
    for where in (y_up, y_down):
        pl.semaphore_signal(barrier, 1, device_id=where, device_id_type=MESH)
    for present, where in peers:
        @pl.when(present)
        def _(where=where):
            pl.semaphore_signal(barrier, 1, device_id=where, device_id_type=MESH)
        expected = expected + jnp.where(present, 1, 0)

    def remote(src, dst, send, recv, where):
        return pltpu.make_async_remote_copy(
            src_ref=src, dst_ref=dst, send_sem=send, recv_sem=recv,
            device_id=where, device_id_type=MESH)

    def x_copies(t):
        return [
            (has_right, has_left, remote(
                cur.at[t, :, cells_x, own, :], cur.at[t, :, 0, own, :],
                xs.at[t, 0], xr.at[t, 0], {"gx": gx + 1})),
            (has_left, has_right, remote(
                cur.at[t, :, 1, own, :], cur.at[t, :, cells_x + 1, own, :],
                xs.at[t, 1], xr.at[t, 1], {"gx": gx - 1})),
        ]

    def y_copies(t):
        return [
            remote(y_send.at[t, 1], y_recv.at[t, 0], ys.at[t, 0], yr.at[t, 0], y_up),
            remote(y_send.at[t, 0], y_recv.at[t, 1], ys.at[t, 1], yr.at[t, 1], y_down),
        ]

    def z_copies(t):
        return [
            (has_above, has_below, remote(
                z_send.at[t], z_low.at[t], zs.at[t, 0], zr.at[t, 0], {"gz": gz + 1})),
            (has_below, has_above, remote(
                z_send.at[t], z_high.at[t], zs.at[t, 1], zr.at[t, 1], {"gz": gz - 1})),
        ]

    lane = lax.broadcasted_iota(jnp.int32, (cells_y, cells_z), 1)

    def pack(t, x, planes, acc):
        for c in range(comps):
            j = c * cells_x + x
            y_send[t, 0, j] = planes[c][0:1, :]
            y_send[t, 1, j] = planes[c][cells_y - 1:cells_y, :]
            turned = pltpu.roll(planes[c], (2 * j + 1) % cells_z, 1)
            acc = jnp.where(lane // 2 == j, turned, acc)
        return acc

    def start_x(t):
        for sends, _, copy in x_copies(t):
            pl.when(sends)(copy.start)

    def start_yz(t):
        for copy in y_copies(t):
            copy.start()
        for sends, _, copy in z_copies(t):
            pl.when(sends)(copy.start)

    edge_rows = jnp.zeros((comps, cells_x, 1, cells_z), jnp.float32)
    for t in range(STEPS):
        cur[t, :, pl.ds(1, cells_x), TOP - 1:TOP, :] = edge_rows
        cur[t, :, pl.ds(1, cells_x), TOP + cells_y:TOP + cells_y + 1, :] = edge_rows

        @pl.when(gx == nx - 1)
        def _(t=t):
            cur[t, :, cells_x + 1, own, :] = jnp.zeros((comps, cells_y, cells_z), jnp.float32)

        @pl.when(gz == 0)
        def _(t=t):
            z_low[t] = jnp.zeros((cells_y, cells_z), jnp.float32)

        @pl.when(gz == nz - 1)
        def _(t=t):
            z_high[t] = jnp.zeros((cells_y, cells_z), jnp.float32)

    load_e.wait()
    load_l.wait()
    weight = blend_ref[0]

    def blended():
        mixed = (1.0 - weight) * early[...] + weight * late[...]
        return jnp.concatenate([mixed] * share, axis=2)

    feed = [remote(inflow_send, inflow_recv.at[k], fs.at[k], fr.at[k], {"gx": 0})
            for k in range(share)]

    @pl.when(feeds)
    def _():
        inflow_send[...] = blended()

    @pl.when((gx == 0) & (gz == 0))
    def _():
        inflow_recv[0] = blended()

    load_v.wait()
    pl.semaphore_wait(barrier, expected)
    start_x(0)

    def first(x, acc):
        return pack(0, x, [cur[0, c, x + 1, own, :] for c in range(comps)], acc)

    zero = jnp.zeros((cells_y, cells_z), jnp.float32)
    z_send[0] = lax.fori_loop(0, cells_x, first, zero, unroll=UNROLL + 1)
    start_yz(0)
    for k in range(share):
        @pl.when(feeds & (lax.rem(gx, share) == k))
        def _(k=k):
            feed[k].start()

    row = lax.broadcasted_iota(jnp.int32, (TOP, cells_z), 0)

    def store(t, c, x, value):
        if t == STEPS:
            out_ref[c, x] = value
        else:
            cur[t, c, x + 1, own, :] = value

    def inner(t, x, left, right):
        q = [cur[t, c, x + 1, own, :] for c in range(comps)]
        ahead, back = [], []
        keep = jnp.float32(1.0)
        for c in range(comps):
            scaled = COURANT * q[c]
            back.append(jnp.maximum(scaled, 0.0))
            ahead.append(back[c] - scaled)
            keep = keep - jnp.abs(scaled)
        back_z = jnp.where(lane == 0, 0.0, back[2])
        ahead_z = jnp.where(lane == cells_z - 1, 0.0, ahead[2])
        for c in range(comps):
            total = (back[1] * cur[t, c, x + 1, pl.ds(TOP - 1, cells_y), :]
                     + ahead[1] * cur[t, c, x + 1, pl.ds(TOP + 1, cells_y), :])
            total += (back_z * pltpu.roll(q[c], 1, 1)
                      + ahead_z * pltpu.roll(q[c], cells_z - 1, 1))
            if left:
                total += back[0] * cur[t, c, x, own, :]
            if right:
                total += ahead[0] * cur[t, c, x + 2, own, :]
            store(t + 1, c, x, keep * q[c] + total)

    def inner_all(t):
        inner(t, 0, False, True)

        def body(x, carry):
            inner(t, x, True, True)
            return carry

        lax.fori_loop(1, cells_x - 1, body, 0, unroll=UNROLL)
        inner(t, cells_x - 1, True, False)

    def finish(t, x, halo, acc, left=False, right=False):
        scaled = COURANT * cur[t, 2, x + 1, own, :]
        weight_z = jnp.where(
            lane == 0, jnp.maximum(scaled, 0.0),
            jnp.where(lane == cells_z - 1, jnp.maximum(-scaled, 0.0), 0.0))
        first_rows = COURANT * cur[t, 1, x + 1, pl.ds(TOP, TOP), :]
        last_rows = COURANT * cur[t, 1, x + 1, pl.ds(cells_y, TOP), :]
        weight_first = jnp.where(row == 0, jnp.maximum(first_rows, 0.0), 0.0)
        weight_last = jnp.where(row == TOP - 1, jnp.maximum(-last_rows, 0.0), 0.0)
        if left:
            weight_x = jnp.maximum(COURANT * cur[t, 0, x + 1, own, :], 0.0)
        if right:
            weight_x = jnp.maximum(-COURANT * cur[t, 0, x + 1, own, :], 0.0)
        planes = []
        for c in range(comps):
            j = c * cells_x + x
            value = out_ref[c, x] if t == STEPS - 1 else cur[t + 1, c, x + 1, own, :]
            value += weight_z * pltpu.roll(halo, (2 * cells_z - 2 * j) % cells_z, 1)
            if left:
                value += weight_x * cur[t, c, x, own, :]
            if right:
                value += weight_x * cur[t, c, x + 2, own, :]
            value = jnp.concatenate([
                value[:TOP] + weight_first * y_recv[t, 0, j],
                value[TOP:cells_y - TOP],
                value[cells_y - TOP:] + weight_last * y_recv[t, 1, j],
            ], axis=0)
            store(t + 1, c, x, value)
            planes.append(value)
        return pack(t + 1, x, planes, acc) if t < STEPS - 1 else acc

    for t in range(STEPS):
        inner_all(t)
        for _, recvs, copy in z_copies(t):
            pl.when(recvs)(copy.wait_recv)
        for copy in y_copies(t):
            copy.wait_recv()
        halo = jnp.where(lane % 2 == 0, z_low[t], pltpu.roll(z_high[t], cells_z - 2, 1))
        for _, recvs, copy in x_copies(t):
            pl.when(recvs)(copy.wait_recv)
        if t == 0:
            @pl.when(gx == 0)
            def _():
                for k in range(share):
                    @pl.when(gz * share + k != 0)
                    def _(k=k):
                        feed[k].wait_recv()
                for c in range(comps):
                    plane = inflow_recv[0, c]
                    for k in range(1, share):
                        plane = jnp.where(lane // piece == k, inflow_recv[k, c], plane)
                    for s in range(STEPS):
                        cur[s, c, 0, own, :] = plane

        acc = finish(t, 0, halo, zero, left=True)
        acc = finish(t, cells_x - 1, halo, acc, right=True)
        if t < STEPS - 1:
            start_x(t + 1)

        def body(x, acc, t=t, halo=halo):
            return finish(t, x, halo, acc)

        acc = lax.fori_loop(1, cells_x - 1, body, acc, unroll=UNROLL)
        if t < STEPS - 1:
            z_send[t + 1] = acc
            start_yz(t + 1)

    for t in range(STEPS):
        for sends, _, copy in x_copies(t):
            pl.when(sends)(copy.wait_send)
        for copy in y_copies(t):
            copy.wait_send()
        for sends, _, copy in z_copies(t):
            pl.when(sends)(copy.wait_send)
    for k in range(share):
        @pl.when(feeds & (lax.rem(gx, share) == k))
        def _(k=k):
            feed[k].wait_send()


def local(sizes, velocity, plane_early, plane_late, blend):
    comps, cells_x, cells_y, cells_z = velocity.shape
    nx, ny, nz = sizes
    assert nx % nz == 0 and cells_z == 128 and 2 * comps * cells_x <= cells_z
    share = nx // nz
    planes = comps * cells_x
    block = (comps, cells_y, cells_z)
    dma = pltpu.SemaphoreType.DMA
    return pl.pallas_call(
        functools.partial(kernel, sizes),
        out_shape=pltpu.VMEM(velocity.shape, velocity.dtype),
        in_specs=[pl.BlockSpec(memory_space=pl.ANY)] * 3
        + [pl.BlockSpec(memory_space=pltpu.SMEM)],
        out_specs=pl.BlockSpec(memory_space=pltpu.VMEM),
        scratch_shapes=[
            pltpu.VMEM((STEPS, comps, cells_x + 2, cells_y + 2 * TOP, cells_z), jnp.float32),
            pltpu.VMEM(plane_early.shape, jnp.float32),
            pltpu.VMEM(plane_late.shape, jnp.float32),
            pltpu.VMEM(block, jnp.float32),
            pltpu.VMEM((share,) + block, jnp.float32),
            pltpu.VMEM((STEPS, 2, planes, 1, cells_z), jnp.float32),
            pltpu.VMEM((STEPS, 2, planes, 1, cells_z), jnp.float32),
            pltpu.VMEM((STEPS, cells_y, cells_z), jnp.float32),
            pltpu.VMEM((STEPS, cells_y, cells_z), jnp.float32),
            pltpu.VMEM((STEPS, cells_y, cells_z), jnp.float32),
            dma((3,)),
            dma((STEPS, 2)), dma((STEPS, 2)),
            dma((STEPS, 2)), dma((STEPS, 2)),
            dma((STEPS, 2)), dma((STEPS, 2)),
            dma((share,)), dma((share,)),
        ],
        compiler_params=pltpu.CompilerParams(collective_id=0, has_side_effects=True),
        name="advect_substeps",
    )(velocity, plane_early, plane_late, blend)


def solution(mesh):
    sizes = tuple(mesh.shape[name] for name in ("gx", "gy", "gz"))
    return jax.shard_map(
        functools.partial(local, sizes),
        mesh=mesh,
        in_specs=(P(None, "gx", "gy", "gz"), P(None, "gy", "gx"), P(None, "gy", "gx"), P()),
        out_specs=P(None, "gx", "gy", "gz"),
        check_vma=False,
    )
```

```python
import functools

import jax
import jax.numpy as jnp
from jax import lax
from jax.experimental import pallas as pl
from jax.experimental.pallas import tpu as pltpu
from jax.sharding import PartitionSpec as P

STEPS = 4
COURANT = 0.08
UNROLL = 7
TOP = 8

MESH = pl.DeviceIdType.MESH


def kernel(sizes, vel_hbm, early_hbm, late_hbm, blend_ref, out_ref,
           cur, early, late, inflow_send, inflow_recv,
           y_send, y_recv, z_send, z_low, z_high,
           load_sem, xs, xr, ys, yr, zs, zr, fs, fr):
    nx, ny, nz = sizes
    comps, cells_x, cells_y, cells_z = vel_hbm.shape
    share = nx // nz
    piece = early_hbm.shape[2]
    gx, gy, gz = (lax.axis_index(name) for name in ("gx", "gy", "gz"))
    own = pl.ds(TOP, cells_y)

    load_v = pltpu.make_async_copy(
        vel_hbm, cur.at[0, :, pl.ds(1, cells_x), own, :], load_sem.at[0])
    load_e = pltpu.make_async_copy(early_hbm, early, load_sem.at[1])
    load_l = pltpu.make_async_copy(late_hbm, late, load_sem.at[2])
    load_e.start()
    load_l.start()
    load_v.start()

    has_left, has_right = gx > 0, gx < nx - 1
    has_below, has_above = gz > 0, gz < nz - 1
    feeds = (gz == gx // share) & (gx != 0)
    y_up = {"gy": lax.rem(gy + 1, ny)}
    y_down = {"gy": lax.rem(gy + ny - 1, ny)}

    barrier = pltpu.get_barrier_semaphore()
    peers = [
        (has_left, {"gx": gx - 1}),
        (has_right, {"gx": gx + 1}),
        (has_below, {"gz": gz - 1}),
        (has_above, {"gz": gz + 1}),
        (feeds, {"gx": 0}),
    ]
    for k in range(share):
        source = gz * share + k
        peers.append(((gx == 0) & (source != 0), {"gx": source}))
    expected = jnp.int32(2)
    for where in (y_up, y_down):
        pl.semaphore_signal(barrier, 1, device_id=where, device_id_type=MESH)
    for present, where in peers:
        @pl.when(present)
        def _(where=where):
            pl.semaphore_signal(barrier, 1, device_id=where, device_id_type=MESH)
        expected = expected + jnp.where(present, 1, 0)

    def remote(src, dst, send, recv, where):
        return pltpu.make_async_remote_copy(
            src_ref=src, dst_ref=dst, send_sem=send, recv_sem=recv,
            device_id=where, device_id_type=MESH)

    def x_copies(t):
        return [
            (has_right, has_left, remote(
                cur.at[t, :, cells_x, own, :], cur.at[t, :, 0, own, :],
                xs.at[t, 0], xr.at[t, 0], {"gx": gx + 1})),
            (has_left, has_right, remote(
                cur.at[t, :, 1, own, :], cur.at[t, :, cells_x + 1, own, :],
                xs.at[t, 1], xr.at[t, 1], {"gx": gx - 1})),
        ]

    def y_copies(t):
        return [
            remote(y_send.at[t, 1], y_recv.at[t, 0], ys.at[t, 0], yr.at[t, 0], y_up),
            remote(y_send.at[t, 0], y_recv.at[t, 1], ys.at[t, 1], yr.at[t, 1], y_down),
        ]

    def z_copies(t):
        return [
            (has_above, has_below, remote(
                z_send.at[t], z_low.at[t], zs.at[t, 0], zr.at[t, 0], {"gz": gz + 1})),
            (has_below, has_above, remote(
                z_send.at[t], z_high.at[t], zs.at[t, 1], zr.at[t, 1], {"gz": gz - 1})),
        ]

    lane = lax.broadcasted_iota(jnp.int32, (cells_y, cells_z), 1)

    def pack(x, planes, acc, rows):
        for c in range(comps):
            j = c * cells_x + x
            turned = pltpu.roll(planes[c], (2 * j + 1) % cells_z, 1)
            acc = jnp.where(lane[rows] // 2 == j, turned, acc)
        return acc

    def edge_row(t, side, c, x, value):
        y_send[t, side, c * cells_x + x] = value

    def start_x(t):
        for sends, _, copy in x_copies(t):
            pl.when(sends)(copy.start)

    def start_y(t):
        for copy in y_copies(t):
            copy.start()

    def start_z(t):
        for sends, _, copy in z_copies(t):
            pl.when(sends)(copy.start)

    edge_rows = jnp.zeros((comps, cells_x, 1, cells_z), jnp.float32)
    for t in range(STEPS):
        cur[t, :, pl.ds(1, cells_x), TOP - 1:TOP, :] = edge_rows
        cur[t, :, pl.ds(1, cells_x), TOP + cells_y:TOP + cells_y + 1, :] = edge_rows

        @pl.when(gx == nx - 1)
        def _(t=t):
            cur[t, :, cells_x + 1, own, :] = jnp.zeros((comps, cells_y, cells_z), jnp.float32)

        @pl.when(gz == 0)
        def _(t=t):
            z_low[t] = jnp.zeros((cells_y, cells_z), jnp.float32)

        @pl.when(gz == nz - 1)
        def _(t=t):
            z_high[t] = jnp.zeros((cells_y, cells_z), jnp.float32)

    load_e.wait()
    load_l.wait()
    weight = blend_ref[0]

    def blended():
        mixed = (1.0 - weight) * early[...] + weight * late[...]
        return jnp.concatenate([mixed] * share, axis=2)

    feed = [remote(inflow_send, inflow_recv.at[k], fs.at[k], fr.at[k], {"gx": 0})
            for k in range(share)]

    @pl.when(feeds)
    def _():
        inflow_send[...] = blended()

    @pl.when((gx == 0) & (gz == 0))
    def _():
        inflow_recv[0] = blended()

    pl.semaphore_wait(barrier, expected)
    for k in range(share):
        @pl.when(feeds & (lax.rem(gx, share) == k))
        def _(k=k):
            feed[k].start()

    load_v.wait()

    def rows_of(x, carry):
        for c in range(comps):
            edge_row(0, 0, c, x, cur[0, c, x + 1, TOP:TOP + 1, :])
            edge_row(0, 1, c, x, cur[0, c, x + 1, TOP + cells_y - 1:TOP + cells_y, :])
        return carry

    lax.fori_loop(0, cells_x, rows_of, 0, unroll=UNROLL + 1)
    start_y(0)
    start_x(0)

    def first(x, acc):
        planes = [cur[0, c, x + 1, own, :] for c in range(comps)]
        return pack(x, planes, acc, slice(None))

    zero = jnp.zeros((cells_y, cells_z), jnp.float32)
    z_send[0] = lax.fori_loop(0, cells_x, first, zero, unroll=UNROLL + 1)
    start_z(0)

    def store(t, c, x, value):
        if t == STEPS:
            out_ref[c, x] = value
        else:
            cur[t, c, x + 1, own, :] = value

    def inner(t, x, left, right):
        q = [cur[t, c, x + 1, own, :] for c in range(comps)]
        ahead, back = [], []
        keep = jnp.float32(1.0)
        for c in range(comps):
            scaled = COURANT * q[c]
            back.append(jnp.maximum(scaled, 0.0))
            ahead.append(back[c] - scaled)
            keep = keep - jnp.abs(scaled)
        back_z = jnp.where(lane == 0, 0.0, back[2])
        ahead_z = jnp.where(lane == cells_z - 1, 0.0, ahead[2])
        for c in range(comps):
            total = (back[1] * cur[t, c, x + 1, pl.ds(TOP - 1, cells_y), :]
                     + ahead[1] * cur[t, c, x + 1, pl.ds(TOP + 1, cells_y), :])
            total += (back_z * pltpu.roll(q[c], 1, 1)
                      + ahead_z * pltpu.roll(q[c], cells_z - 1, 1))
            if left:
                total += back[0] * cur[t, c, x, own, :]
            if right:
                total += ahead[0] * cur[t, c, x + 2, own, :]
            store(t + 1, c, x, keep * q[c] + total)

    def inner_all(t):
        inner(t, 0, False, True)

        def body(x, carry):
            inner(t, x, True, True)
            return carry

        lax.fori_loop(1, cells_x - 1, body, 0, unroll=UNROLL)
        inner(t, cells_x - 1, True, False)

    middle = slice(TOP, cells_y - TOP)
    low, high = slice(0, TOP), slice(cells_y - TOP, cells_y)

    def partly(t, x, halo, acc, left=False, right=False):
        scaled = COURANT * cur[t, 2, x + 1, own, :]
        weight_z = jnp.where(
            lane == 0, jnp.maximum(scaled, 0.0),
            jnp.where(lane == cells_z - 1, jnp.maximum(-scaled, 0.0), 0.0))
        if left:
            weight_x = jnp.maximum(COURANT * cur[t, 0, x + 1, own, :], 0.0)
        if right:
            weight_x = jnp.maximum(-COURANT * cur[t, 0, x + 1, own, :], 0.0)
        planes = []
        for c in range(comps):
            j = c * cells_x + x
            value = out_ref[c, x] if t == STEPS - 1 else cur[t + 1, c, x + 1, own, :]
            value += weight_z * pltpu.roll(halo, (2 * cells_z - 2 * j) % cells_z, 1)
            if left:
                value += weight_x * cur[t, c, x, own, :]
            if right:
                value += weight_x * cur[t, c, x + 2, own, :]
            store(t + 1, c, x, value)
            planes.append(value[middle])
        return pack(x, planes, acc, middle) if t < STEPS - 1 else acc

    def edges(t, x, carry):
        weights = (jnp.maximum(COURANT * cur[t, 1, x + 1, TOP:TOP + 1, :], 0.0),
                   jnp.maximum(-COURANT * cur[t, 1, x + 1, TOP + cells_y - 1:TOP + cells_y, :], 0.0))
        for c in range(comps):
            for side, y in enumerate((0, cells_y - 1)):
                term = weights[side] * y_recv[t, side, c * cells_x + x]
                if t == STEPS - 1:
                    out_ref[c, x, y:y + 1, :] += term
                else:
                    value = cur[t + 1, c, x + 1, TOP + y:TOP + y + 1, :] + term
                    cur[t + 1, c, x + 1, TOP + y:TOP + y + 1, :] = value
                    edge_row(t + 1, side, c, x, value)
        return carry

    some = jnp.zeros((cells_y - 2 * TOP, cells_z), jnp.float32)
    few = jnp.zeros((TOP, cells_z), jnp.float32)
    for t in range(STEPS):
        inner_all(t)
        for _, recvs, copy in z_copies(t):
            pl.when(recvs)(copy.wait_recv)
        halo = jnp.where(lane % 2 == 0, z_low[t], pltpu.roll(z_high[t], cells_z - 2, 1))

        def body(x, acc, t=t, halo=halo):
            return partly(t, x, halo, acc)

        acc = lax.fori_loop(1, cells_x - 1, body, some, unroll=UNROLL)
        for _, recvs, copy in x_copies(t):
            pl.when(recvs)(copy.wait_recv)
        if t == 0:
            @pl.when(gx == 0)
            def _():
                for k in range(share):
                    @pl.when(gz * share + k != 0)
                    def _(k=k):
                        feed[k].wait_recv()
                for c in range(comps):
                    plane = inflow_recv[0, c]
                    for k in range(1, share):
                        plane = jnp.where(lane // piece == k, inflow_recv[k, c], plane)
                    for s in range(STEPS):
                        cur[s, c, 0, own, :] = plane

        acc = partly(t, 0, halo, acc, left=True)
        acc = partly(t, cells_x - 1, halo, acc, right=True)
        for copy in y_copies(t):
            copy.wait_recv()

        def rows(x, carry, t=t):
            return edges(t, x, carry)

        lax.fori_loop(0, cells_x, rows, 0, unroll=UNROLL + 1)
        if t < STEPS - 1:
            start_y(t + 1)
            start_x(t + 1)

            def ends(x, accs, t=t):
                top = [cur[t + 1, c, x + 1, pl.ds(TOP, TOP), :] for c in range(comps)]
                last = [cur[t + 1, c, x + 1, pl.ds(cells_y, TOP), :] for c in range(comps)]
                return pack(x, top, accs[0], low), pack(x, last, accs[1], high)

            top, last = lax.fori_loop(0, cells_x, ends, (few, few), unroll=UNROLL + 1)
            z_send[t + 1] = jnp.concatenate([top, acc, last], axis=0)
            start_z(t + 1)

    for t in range(STEPS):
        for sends, _, copy in x_copies(t):
            pl.when(sends)(copy.wait_send)
        for copy in y_copies(t):
            copy.wait_send()
        for sends, _, copy in z_copies(t):
            pl.when(sends)(copy.wait_send)
    for k in range(share):
        @pl.when(feeds & (lax.rem(gx, share) == k))
        def _(k=k):
            feed[k].wait_send()


def local(sizes, velocity, plane_early, plane_late, blend):
    comps, cells_x, cells_y, cells_z = velocity.shape
    nx, ny, nz = sizes
    assert nx % nz == 0 and cells_z == 128 and 2 * comps * cells_x <= cells_z
    share = nx // nz
    planes = comps * cells_x
    block = (comps, cells_y, cells_z)
    dma = pltpu.SemaphoreType.DMA
    return pl.pallas_call(
        functools.partial(kernel, sizes),
        out_shape=pltpu.VMEM(velocity.shape, velocity.dtype),
        in_specs=[pl.BlockSpec(memory_space=pl.ANY)] * 3
        + [pl.BlockSpec(memory_space=pltpu.SMEM)],
        out_specs=pl.BlockSpec(memory_space=pltpu.VMEM),
        scratch_shapes=[
            pltpu.VMEM((STEPS, comps, cells_x + 2, cells_y + 2 * TOP, cells_z), jnp.float32),
            pltpu.VMEM(plane_early.shape, jnp.float32),
            pltpu.VMEM(plane_late.shape, jnp.float32),
            pltpu.VMEM(block, jnp.float32),
            pltpu.VMEM((share,) + block, jnp.float32),
            pltpu.VMEM((STEPS, 2, planes, 1, cells_z), jnp.float32),
            pltpu.VMEM((STEPS, 2, planes, 1, cells_z), jnp.float32),
            pltpu.VMEM((STEPS, cells_y, cells_z), jnp.float32),
            pltpu.VMEM((STEPS, cells_y, cells_z), jnp.float32),
            pltpu.VMEM((STEPS, cells_y, cells_z), jnp.float32),
            dma((3,)),
            dma((STEPS, 2)), dma((STEPS, 2)),
            dma((STEPS, 2)), dma((STEPS, 2)),
            dma((STEPS, 2)), dma((STEPS, 2)),
            dma((share,)), dma((share,)),
        ],
        compiler_params=pltpu.CompilerParams(collective_id=0, has_side_effects=True),
        name="advect_substeps",
    )(velocity, plane_early, plane_late, blend)


def solution(mesh):
    sizes = tuple(mesh.shape[name] for name in ("gx", "gy", "gz"))
    return jax.shard_map(
        functools.partial(local, sizes),
        mesh=mesh,
        in_specs=(P(None, "gx", "gy", "gz"), P(None, "gy", "gx"), P(None, "gy", "gx"), P()),
        out_specs=P(None, "gx", "gy", "gz"),
        check_vma=False,
    )
```
